16 devices in a mesh: rep: 2 (over y, z), dp: 8 (over x, core).
Axes of the slice: x: 4, y: 2, z: 1, core: 2. Of those that a mesh axis runs over, the one named last changes fastest.
The devices are a block of a 4x4x8 slice.
Arguments:
- x: bfloat16 [16, 2048, 1152], P(('rep', 'dp')), parts along dimension 0
- dy: bfloat16 [16, 2048, 1152], P(('rep', 'dp')), parts along dimension 0
- w_gate: bfloat16 [2, 1152, 4608], replicated
- w_up: bfloat16 [2, 1152, 4608], replicated
- w_down: bfloat16 [2, 4608, 1152], replicated
- m_w_gate: float32 [2, 1152, 4608], P(None, 'dp')
- m_w_up: float32 [2, 1152, 4608], P(None, 'dp')
- m_w_down: float32 [2, 4608, 1152], P(None, 'dp')
- v_w_gate: float32 [2, 1152, 4608], P(None, 'dp')
- v_w_up: float32 [2, 1152, 4608], P(None, 'dp')
- v_w_down: float32 [2, 4608, 1152], P(None, 'dp')
Outputs:
- output 1: bfloat16 [4, 1152, 4608], P('rep'), parts along dimension 0
- output 2: bfloat16 [4, 1152, 4608], P('rep'), parts along dimension 0
- output 3: bfloat16 [4, 4608, 1152], P('rep'), parts along dimension 0
- output 4: float32 [4, 1152, 4608], P('rep', 'dp'), parts along dimension 0
- output 5: float32 [4, 1152, 4608], P('rep', 'dp'), parts along dimension 0
- output 6: float32 [4, 4608, 1152], P('rep', 'dp'), parts along dimension 0
- output 7: float32 [4, 1152, 4608], P('rep', 'dp'), parts along dimension 0
- output 8: float32 [4, 1152, 4608], P('rep', 'dp'), parts along dimension 0
- output 9: float32 [4, 4608, 1152], P('rep', 'dp'), parts along dimension 0
There are 2 independent parts. The reference program is written for one: setup_inputs(seed, part) draws one part's arguments, and reference() takes and returns one part's arrays. A program takes and returns all parts, laid end to end along the dimension named above; an argument that names none is the same for every part.
All inputs are finite; a program needn't handle non-finite values.
Results may differ from the reference program's by a relative error of at most 0.022.
Values are sent between devices in bfloat16 or wider.
A program may use at most 768 MiB of HBM per device.

```python
import jax
import jax.numpy as jnp
from jax import lax

SEQUENCES = 8
TOKENS = 2048
D = 1152
FF = 4608
LAYERS = 2
NAMES = ("w_gate", "w_up", "w_down")
SHAPES = {"w_gate": (LAYERS, D, FF), "w_up": (LAYERS, D, FF), "w_down": (LAYERS, FF, D)}


def bump(key, n, height):
    away = (jnp.arange(n, dtype=jnp.int32) - jax.random.randint(key, (), 0, n, jnp.int32)) % n
    return jnp.where(away < n // 8, height, 1.0)


def together(key, own, strength):
    shared = jax.random.normal(key, own.shape[1:], jnp.float32)
    return (own + strength * shared) * lax.rsqrt(1 + strength * strength)


def setup_inputs(seed: int = 0, part: int = 0) -> dict:
    kx, kdy, ka, kb, kz, kf, kh, kl, *keys = jax.random.split(jax.random.key(seed), 8 + 3 * len(NAMES))
    kx, kdy, ka, kb = (jax.random.fold_in(k, part) for k in (kx, kdy, ka, kb))
    kw, km, kv = (keys[i::3] for i in range(3))
    shape = (SEQUENCES, TOKENS, D)
    much_x, much_dy = jax.random.uniform(kz, (2,), jnp.float32, 0.0, 1.0)
    loud = 2.0 ** jax.random.uniform(jax.random.fold_in(kz, 1), (), jnp.float32, -1.0, 2.0)
    layers = 2.0 ** jax.random.uniform(kl, (LAYERS, 1, 1), jnp.float32, -1.0, 1.0)
    x = together(ka, jax.random.normal(kx, shape, jnp.float32), much_x) * bump(kf, D, 4.0)
    dy = together(kb, jax.random.normal(kdy, shape, jnp.float32), much_dy)
    drawn = {"x": x.astype(jnp.bfloat16), "dy": (loud * dy * (SEQUENCES * TOKENS) ** -0.5).astype(jnp.bfloat16)}
    for key, name in zip(kw, NAMES, strict=True):
        w = jax.random.normal(key, SHAPES[name], jnp.float32) * SHAPES[name][1] ** -0.5
        drawn[name] = (w * {"w_gate": 1.0, "w_up": bump(kh, FF, 4.0), "w_down": layers}[name]).astype(jnp.bfloat16)
    for key, name in zip(km, NAMES, strict=True):
        drawn[f"m_{name}"] = 0.1 * jax.random.normal(key, SHAPES[name], jnp.float32)
    for key, name in zip(kv, NAMES, strict=True):
        drawn[f"v_{name}"] = jax.random.uniform(key, SHAPES[name], jnp.float32, 0.005, 0.015)
    return drawn


def matmul(a, w):
    return jnp.dot(a, w, preferred_element_type=jnp.float32).astype(jnp.bfloat16)


def normed(h):
    wide = h.astype(jnp.float32)
    scale = lax.rsqrt(jnp.mean(wide**2, -1, keepdims=True) + 1e-6)
    return (wide * scale).astype(jnp.bfloat16)


def layer(h, w):
    a = normed(h)
    gate = jnp.dot(a, w["w_gate"], preferred_element_type=jnp.float32)
    up = jnp.dot(a, w["w_up"], preferred_element_type=jnp.float32)
    return h + matmul((jax.nn.silu(gate) * up).astype(jnp.bfloat16), w["w_down"])


def adamw(w, m, v, g):
    m = 0.9 * m + 0.1 * g
    v = 0.95 * v + 0.05 * g * g
    step = m * lax.rsqrt(v + 1e-8) + 0.1 * w
    return (w - 0.02 * step).astype(jnp.bfloat16), m, v


def clipped(gradients, sum_of_squares, count):
    factor = jnp.minimum(1.0, 0.5 * lax.rsqrt(sum_of_squares / count + 1e-30))
    return [g * factor for g in gradients]


def stack(weights, h):
    return lax.scan(lambda h, w: (layer(h, w), None), h, weights)[0]


def reference(x, dy, w_gate, w_up, w_down, m_w_gate, m_w_up, m_w_down, v_w_gate, v_w_up, v_w_down):
    weights = dict(zip(NAMES, (w_gate, w_up, w_down), strict=True))

    def take(so_far, sequence):
        h, by_y = sequence
        _, back = jax.vjp(lambda w: stack(w, h), weights)
        return jax.tree.map(lambda total, term: total + term.astype(jnp.float32), so_far, back(by_y)[0]), None

    none_yet = {name: jnp.zeros(w.shape, jnp.float32) for name, w in weights.items()}
    by_weights, _ = lax.scan(take, none_yet, (x, dy))
    gradients = [by_weights[name].astype(jnp.bfloat16).astype(jnp.float32) for name in NAMES]
    gradients = clipped(gradients, sum(jnp.sum(g * g) for g in gradients), sum(g.size for g in gradients))
    new = [
        adamw(w.astype(jnp.float32), m, v, g)
        for w, m, v, g in zip((w_gate, w_up, w_down), (m_w_gate, m_w_up, m_w_down), (v_w_gate, v_w_up, v_w_down), gradients, strict=True)
    ]
    return tuple(one[which] for which in range(3) for one in new)
```

```python
import functools

import jax
import jax.numpy as jnp
from jax import lax
from jax.experimental import pallas as pl
from jax.experimental.pallas import tpu as pltpu
from jax.sharding import PartitionSpec as P

BF, F32 = jnp.bfloat16, jnp.float32
LANES = 128
MESH = pl.DeviceIdType.MESH
NN, NT, TN = ((1,), (0,)), ((1,), (1,)), ((0,), (0,))
VMEM_LIMIT = 67_000_000


def dot(a, b, dims):
    return lax.dot_general(a, b, (dims, ((), ())), preferred_element_type=F32)


def rows_of(i, n):
    return pl.ds(pl.multiple_of(i * n, n), n)


def scale_of(wide):
    return lax.rsqrt(jnp.mean(wide * wide, -1, keepdims=True) + 1e-6)


class Sizes:
    def __init__(self, mesh, x, w_gate):
        self.axes = mesh.axis_names
        self.devices = mesh.shape["dp"]
        self.chips = self.devices // 2
        self.tokens, self.d = x.shape[-2:]
        self.ff = w_gate.shape[-1]
        self.block = LANES * self.chips
        self.blocks = self.ff // self.block
        self.rows = self.d // self.devices
        self.down_rows = LANES // 2

    def tile(self, chip, b):
        return pl.multiple_of((self.blocks * chip + b) * LANES, LANES)


def forward_kernel(z, tm, layer, x_hbm, wg, wu, wd, h_out, a_out, a0_out, act_out, slope_out, p_out,
                   x_v, a_v, p_v, wg_v, wu_v, wd_v, act_v, slope_v, in_sem, wg_sem, wu_sem, wd_sem, act_sem, slope_sem, p_sem, out_sem):
    def fetch(b, slot):
        for c in range(z.chips):
            cols = slice(c * LANES, (c + 1) * LANES)
            pltpu.make_async_copy(wg.at[layer, :, pl.ds(z.tile(c, b), LANES)], wg_v.at[slot, :, cols], wg_sem.at[slot]).start()
            pltpu.make_async_copy(wu.at[layer, :, pl.ds(z.tile(c, b), LANES)], wu_v.at[slot, :, cols], wu_sem.at[slot]).start()

    load = pltpu.make_async_copy(x_hbm, x_v, in_sem)
    load.start()
    fetch(0, 0)
    for b in range(z.blocks):
        for c in range(z.chips):
            to = b * z.block + c * LANES
            pltpu.make_async_copy(wd.at[layer, pl.ds(z.tile(c, b), LANES), :], wd_v.at[to : to + LANES, :], wd_sem).start()
    load.wait()

    def norm(i, _):
        r = rows_of(i, 256)
        wide = x_v[r, :].astype(F32)
        a_v[r, :] = (wide * scale_of(wide)).astype(BF)
        return 0

    lax.fori_loop(0, z.tokens // 256, norm, 0)
    keep_a = pltpu.make_async_copy(a_v, a0_out, out_sem.at[0])
    keep_a.start()
    tiles = z.tokens // tm

    def stores(b, i, s):
        r = rows_of(i, tm)
        return (
            pltpu.make_async_copy(act_v.at[s], act_out.at[b, r, :], act_sem.at[s]),
            pltpu.make_async_copy(slope_v.at[s], slope_out.at[b, r, :], slope_sem.at[s]),
        )

    def block(b, _):
        slot = lax.rem(b, 2)
        pltpu.make_async_copy(wg_v.at[slot], wg_v.at[slot], wg_sem.at[slot]).wait()
        pltpu.make_async_copy(wu_v.at[slot], wu_v.at[slot], wu_sem.at[slot]).wait()

        @pl.when(b + 1 < z.blocks)
        def _():
            fetch(b + 1, 1 - slot)

        cols = pl.ds(pl.multiple_of(b * z.block, z.block), z.block)

        def pair(j, _):
            for s in range(2):
                i = 2 * j + s
                r = rows_of(i, tm)
                gate = dot(a_v[r, :], wg_v[slot], NN)
                up = dot(a_v[r, :], wu_v[slot], NN)
                s_ = 1.0 / (1.0 + jnp.exp(-gate))
                act = gate * s_

                @pl.when(b + j > 0)
                def _():
                    for cp in stores(b, i, s):
                        cp.wait()

                p_v[r, cols] = (act * up).astype(BF)
                act_v[s] = act
                slope_v[s] = up * (s_ + act * (1.0 - s_))
                for cp in stores(b, i, s):
                    cp.start()
            return 0

        lax.fori_loop(0, tiles // 2, pair, 0)
        pltpu.make_async_copy(p_v.at[:, cols], p_out.at[b], p_sem.at[b]).start()
        return 0

    lax.fori_loop(0, z.blocks, block, 0)
    for s in range(2):
        for cp in stores(0, 0, s):
            cp.wait()
    pltpu.make_async_copy(wd_v, wd_v, wd_sem).wait()
    keep_a.wait()

    def down(i, _):
        r = rows_of(i, tm)
        out = dot(p_v[r, :], wd_v[...], NN).astype(BF)
        h = (x_v[r, :].astype(F32) + out.astype(F32)).astype(BF)
        x_v[r, :] = h
        wide = h.astype(F32)
        a_v[r, :] = (wide * scale_of(wide)).astype(BF)
        return 0

    lax.fori_loop(0, tiles, down, 0)
    last = (pltpu.make_async_copy(x_v, h_out, out_sem.at[1]), pltpu.make_async_copy(a_v, a_out, out_sem.at[2]))
    for cp in last:
        cp.start()
    for b in range(z.blocks):
        pltpu.make_async_copy(p_v.at[:, b * z.block : (b + 1) * z.block], p_out.at[b], p_sem.at[b]).wait()
    for cp in last:
        cp.wait()


def forward(z, layer, x, wg, wu, wd):
    tm = z.tokens // 4
    t, d, f, n = z.tokens, z.d, z.block, z.blocks
    any_ = pl.BlockSpec(memory_space=pl.ANY)
    sem = pltpu.SemaphoreType.DMA
    return pl.pallas_call(
        functools.partial(forward_kernel, z, tm, layer),
        out_shape=[jax.ShapeDtypeStruct((t, d), BF)] * 3
        + [jax.ShapeDtypeStruct((n, t, f), F32)] * 2
        + [jax.ShapeDtypeStruct((n, t, f), BF)],
        in_specs=[any_] * 4,
        out_specs=[any_] * 6,
        scratch_shapes=[
            pltpu.VMEM((t, d), BF),
            pltpu.VMEM((t, d), BF),
            pltpu.VMEM((t, z.ff), BF),
            pltpu.VMEM((2, d, f), BF),
            pltpu.VMEM((2, d, f), BF),
            pltpu.VMEM((z.ff, d), BF),
            pltpu.VMEM((2, tm, f), F32),
            pltpu.VMEM((2, tm, f), F32),
            sem, sem((2,)), sem((2,)), sem, sem((2,)), sem((2,)), sem((n,)), sem((3,)),
        ],
        compiler_params=pltpu.CompilerParams(vmem_limit_bytes=VMEM_LIMIT),
        cost_estimate=pl.CostEstimate(flops=6 * t * d * z.ff, bytes_accessed=150_000_000, transcendentals=t * z.ff),
        name="forward",
    )(x, wg, wu, wd)


class Ring:
    def scratch(self, z):
        r, f, dr, d, n = z.rows, z.block, z.down_rows, z.d, z.chips
        sem = pltpu.SemaphoreType.DMA
        return dict(
            st_gu=pltpu.VMEM((2, 2, n, 2, r, f), BF),
            st_d=pltpu.VMEM((2, n, 2, dr, d), BF),
            r0_gu=pltpu.VMEM((2, 2, n, r, f), BF),
            r0_d=pltpu.VMEM((2, n, dr, d), BF),
            s_gu=pltpu.VMEM((2, 3, 2, r, f), F32),
            s_d=pltpu.VMEM((2, 3, dr, d), F32),
            t1_gu=pltpu.VMEM((2, r, f), BF),
            t1_d=pltpu.VMEM((2, dr // 2, d), BF),
            r1_gu=pltpu.VMEM((2, 2, r, f), BF),
            r1_d=pltpu.VMEM((2, 2, dr // 2, d), BF),
            t2_gu=pltpu.VMEM((2, 2, r, f), BF),
            t2_d=pltpu.VMEM((2, dr, d), BF),
            r2_gu=pltpu.VMEM((2, 2, 2, r, f), BF),
            r2_d=pltpu.VMEM((2, 2, dr, d), BF),
            sq=pltpu.VMEM((8, LANES), F32),
            sem0=sem((2, 2, 2)),
            sem1=sem((2, 2, 2, 2)),
            sem2=sem((2, 2, 2, 2)),
            swap_sem=sem((2,)),
        )

    def __init__(self, z, out_gu, out_d, from_d, scr):
        self.z, self.out_gu, self.out_d, self.from_d = z, out_gu, out_d, from_d
        self.__dict__.update(scr)
        me = lax.axis_index("dp")
        self.chip, self.core = me // 2, lax.rem(me, 2)
        n = z.chips
        self.right = lax.rem(self.chip + 1, n)
        self.left = lax.rem(self.chip + n - 1, n)
        self.far = lax.rem(self.chip + 2, n)
        self.partner = {"dp": 2 * self.chip + 1 - self.core}
        self.sides = ({"dp": 2 * self.right + self.core}, {"dp": 2 * self.left + self.core})

    def greet(self, everyone):
        barrier = pltpu.get_barrier_semaphore()
        if everyone:
            me = lax.axis_index("dp")
            for i in range(1, self.z.devices):
                pl.semaphore_signal(barrier, inc=1, device_id={"dp": lax.rem(me + i, self.z.devices)}, device_id_type=MESH)
            pl.semaphore_wait(barrier, self.z.devices - 1)
        else:
            for who in (self.partner, *self.sides):
                pl.semaphore_signal(barrier, inc=1, device_id=who, device_id_type=MESH)
            pl.semaphore_wait(barrier, 3)
        self.sq[...] = jnp.zeros_like(self.sq)

    def remote(self, src, dst, sems, who):
        return pltpu.make_async_remote_copy(src, dst, sems.at[0], sems.at[1], device_id=who, device_id_type=MESH)

    def copies0(self, s):
        other = 1 - self.core
        return (
            self.remote(self.st_gu.at[s, :, :, other], self.r0_gu.at[s], self.sem0.at[s, 0], self.partner),
            self.remote(self.st_d.at[s, :, other], self.r0_d.at[s], self.sem0.at[s, 1], self.partner),
        )

    def copies1(self, s):
        out = []
        for way in range(2):
            out.append(self.remote(self.t1_gu.at[way], self.r1_gu.at[s, way], self.sem1.at[s, way, 0], self.sides[way]))
            out.append(self.remote(self.t1_d.at[way], self.r1_d.at[s, way], self.sem1.at[s, way, 1], self.sides[way]))
        return out

    def copies2(self, s):
        out = []
        for way in range(2):
            out.append(self.remote(self.t2_gu.at[way], self.r2_gu.at[s, way], self.sem2.at[s, way, 0], self.sides[way]))
            out.append(self.remote(self.t2_d.at[way], self.r2_d.at[s, way], self.sem2.at[s, way, 1], self.sides[way]))
        return out

    def stage0(self, u):
        for cp in self.copies0(lax.rem(u, 2)):
            cp.start()

    def stage1(self, u):
        s = lax.rem(u, 2)
        for cp in self.copies0(s):
            cp.wait()

        @pl.when(u > 0)
        def _():
            for cp in self.copies1(1 - s):
                cp.wait_send()

        k = self.core
        for at, chip in enumerate((self.right, self.left, self.chip)):
            for w in range(2):
                self.s_gu[s, at, w] = self.st_gu[s, w, chip, k].astype(F32) + self.r0_gu[s, w, chip].astype(F32)
            self.s_d[s, at] = self.st_d[s, chip, k].astype(F32) + self.r0_d[s, chip].astype(F32)
        half = self.z.down_rows // 2
        for w in range(2):
            self.t1_gu[w] = (self.st_gu[s, w, self.far, k].astype(F32) + self.r0_gu[s, w, self.far].astype(F32)).astype(BF)
            h = slice(w * half, (w + 1) * half)
            self.t1_d[w] = (self.st_d[s, self.far, k, h].astype(F32) + self.r0_d[s, self.far, h].astype(F32)).astype(BF)
        for cp in self.copies1(s):
            cp.start()

    def stage2(self, u):
        s = lax.rem(u, 2)
        for cp in self.copies1(s):
            cp.wait_recv()

        @pl.when(u > 0)
        def _():
            for cp in self.copies2(1 - s):
                cp.wait_send()

        half = self.z.down_rows // 2
        for way in range(2):
            w, v = way, 1 - way
            self.t2_gu[way, w] = (self.s_gu[s, way, w] + self.r1_gu[s, way].astype(F32)).astype(BF)
            self.t2_gu[way, v] = self.s_gu[s, way, v].astype(BF)
            h, o = slice(w * half, (w + 1) * half), slice(v * half, (v + 1) * half)
            self.t2_d[way, h] = (self.s_d[s, way, h] + self.r1_d[s, way].astype(F32)).astype(BF)
            self.t2_d[way, o] = self.s_d[s, way, o].astype(BF)
        for cp in self.copies2(s):
            cp.start()

    def stage3(self, u):
        z, s = self.z, lax.rem(u, 2)
        for cp in self.copies2(s):
            cp.wait_recv()

        def count(g):
            wide = g.astype(F32)
            sq = wide * wide
            return jnp.sum(sq.reshape(-1, 8, sq.shape[-1] // LANES, LANES), axis=(0, 2)) if False else self.fold(sq)

        total = self.sq[...]
        for w in range(2):
            g = (self.s_gu[s, 2, w] + self.r2_gu[s, 0, w].astype(F32) + self.r2_gu[s, 1, w].astype(F32)).astype(BF)
            for c in range(z.chips):
                self.out_gu[w, :, pl.ds(z.tile(c, u), LANES)] = g[:, c * LANES : (c + 1) * LANES]
            total += count(g)
        g = (self.s_d[s, 2] + self.r2_d[s, 0].astype(F32) + self.r2_d[s, 1].astype(F32)).astype(BF)
        self.out_d[rows_of(u, z.down_rows), :] = g
        self.sq[...] = total + count(g)

    @staticmethod
    def fold(sq):
        total = jnp.zeros((8, LANES), F32)
        for i in range(0, sq.shape[0], 8):
            for j in range(0, sq.shape[1], LANES):
                total += sq[i : i + 8, j : j + LANES]
        return total

    def tick(self, t):
        n = self.z.blocks
        pl.when(t >= 3)(lambda: self.stage3(t - 3))
        pl.when((t >= 2) & (t < n + 2))(lambda: self.stage2(t - 2))
        pl.when((t >= 1) & (t < n + 1))(lambda: self.stage1(t - 1))
        pl.when(t < n)(lambda: self.stage0(t))

    def finish(self):
        z = self.z
        last = (z.blocks - 1) % 2
        for cp in self.copies1(last):
            cp.wait_send()
        for cp in self.copies2(last):
            cp.wait_send()
        give = z.blocks // 2 * z.down_rows
        at = pl.multiple_of((1 - self.core) * (z.blocks * z.down_rows - give), z.down_rows)
        swap = self.remote(self.out_d.at[pl.ds(at, give), :], self.from_d, self.swap_sem, self.partner)
        swap.start()
        swap.wait()


RING_NAMES = ("st_gu", "st_d", "r0_gu", "r0_d", "s_gu", "s_d", "t1_gu", "t1_d", "r1_gu", "r1_d", "t2_gu", "t2_d", "r2_gu", "r2_d",
              "sq", "sem0", "sem1", "sem2", "swap_sem")


def ring_scratch(z):
    made = Ring.scratch(None, z)
    return [made[name] for name in RING_NAMES]


def shard_shapes(z):
    give = z.blocks // 2 * z.down_rows
    return [
        jax.ShapeDtypeStruct((2, z.rows, z.ff), BF),
        jax.ShapeDtypeStruct((z.blocks * z.down_rows, z.d), BF),
        jax.ShapeDtypeStruct((give, z.d), BF),
    ]


def weight_gradients(z, ring, s, a_v, y_v, p, gg, gu):
    n = z.chips
    ring.st_d[s] = dot(p, y_v[...], TN).astype(BF).reshape(n, 2, z.down_rows, z.d)
    ring.st_gu[s, 0] = dot(a_v[...], gg, TN).astype(BF).reshape(n, 2, z.rows, z.block)
    ring.st_gu[s, 1] = dot(a_v[...], gu, TN).astype(BF).reshape(n, 2, z.rows, z.block)


def last_kernel(z, tm, layer, a_hbm, y_hbm, h_hbm, wg, wu, wd, dh_out, gu_out, d_out, from_d, sq_out,
                a_v, y_v, da_v, p_v, gg_v, gu_v, wg_v, wu_v, wd_v, in_sem, wg_sem, wu_sem, wd_sem, *ring_refs):
    ring = Ring(z, gu_out, d_out, from_d, dict(zip(RING_NAMES, ring_refs, strict=True)))

    def fetch(b, slot):
        for c in range(z.chips):
            cols = slice(c * LANES, (c + 1) * LANES)
            pltpu.make_async_copy(wg.at[layer, :, pl.ds(z.tile(c, b), LANES)], wg_v.at[slot, :, cols], wg_sem.at[slot]).start()
            pltpu.make_async_copy(wu.at[layer, :, pl.ds(z.tile(c, b), LANES)], wu_v.at[slot, :, cols], wu_sem.at[slot]).start()
            pltpu.make_async_copy(wd.at[layer, pl.ds(z.tile(c, b), LANES), :], wd_v.at[slot, cols, :], wd_sem.at[slot]).start()

    loads = (pltpu.make_async_copy(a_hbm, a_v, in_sem.at[0]), pltpu.make_async_copy(y_hbm, y_v, in_sem.at[1]))
    for cp in loads:
        cp.start()
    fetch(0, 0)
    ring.greet(False)
    da_v[...] = jnp.zeros_like(da_v)
    for cp in loads:
        cp.wait()

    def compute(b):
        slot = lax.rem(b, 2)
        for v, sem in ((wg_v, wg_sem), (wu_v, wu_sem), (wd_v, wd_sem)):
            pltpu.make_async_copy(v.at[slot], v.at[slot], sem.at[slot]).wait()

        @pl.when(b + 1 < z.blocks)
        def _():
            fetch(b + 1, 1 - slot)

        def hidden(i, _):
            r = rows_of(i, tm)
            gate = dot(a_v[r, :], wg_v[slot], NN)
            up = dot(a_v[r, :], wu_v[slot], NN)
            dp = dot(y_v[r, :], wd_v[slot], NT).astype(BF).astype(F32)
            s_ = 1.0 / (1.0 + jnp.exp(-gate))
            act = gate * s_
            p_v[r, :] = (act * up).astype(BF)
            gu_v[r, :] = (dp * act).astype(BF)
            gg_v[r, :] = (dp * (up * (s_ + act * (1.0 - s_)))).astype(BF)
            return 0

        lax.fori_loop(0, z.tokens // tm, hidden, 0)
        weight_gradients(z, ring, slot, a_v, y_v, p_v[...], gg_v[...], gu_v[...])

        def back(i, _):
            r = rows_of(i, tm)
            da_v[r, :] += dot(gg_v[r, :], wg_v[slot], NT) + dot(gu_v[r, :], wu_v[slot], NT)
            return 0

        lax.fori_loop(0, z.tokens // tm, back, 0)

    def through_norm():
        load = pltpu.make_async_copy(h_hbm, a_v, in_sem.at[0])
        load.start()
        load.wait()

        def part(i, _):
            r = rows_of(i, 256)
            wide = a_v[r, :].astype(F32)
            scale = scale_of(wide)
            da = da_v[r, :].astype(BF).astype(F32)
            pull = jnp.sum(da * wide, -1, keepdims=True) * (scale * scale * scale) * (1.0 / z.d)
            dh = (da * scale - wide * pull).astype(BF)
            a_v[r, :] = (y_v[r, :].astype(F32) + dh.astype(F32)).astype(BF)
            return 0

        lax.fori_loop(0, z.tokens // 256, part, 0)
        pltpu.make_async_copy(a_v, dh_out, in_sem.at[0]).start()

    def step(t, _):
        pl.when(t < z.blocks)(lambda: compute(t))
        ring.tick(t)
        pl.when(t == z.blocks)(through_norm)
        return 0

    lax.fori_loop(0, z.blocks + 3, step, 0)
    ring.finish()
    sq_out[...] = ring.sq[...]
    pltpu.make_async_copy(a_v, dh_out, in_sem.at[0]).wait()


def last_layer(z, layer, a, y, h, wg, wu, wd):
    tm = z.tokens // 4
    t, d, f = z.tokens, z.d, z.block
    any_, vmem = pl.BlockSpec(memory_space=pl.ANY), pl.BlockSpec(memory_space=pltpu.VMEM)
    sem = pltpu.SemaphoreType.DMA
    return pl.pallas_call(
        functools.partial(last_kernel, z, tm, layer),
        out_shape=[jax.ShapeDtypeStruct((t, d), BF)] + shard_shapes(z) + [jax.ShapeDtypeStruct((8, LANES), F32)],
        in_specs=[any_] * 6,
        out_specs=[any_] + [vmem] * 4,
        scratch_shapes=[
            pltpu.VMEM((t, d), BF),
            pltpu.VMEM((t, d), BF),
            pltpu.VMEM((t, d), F32),
            pltpu.VMEM((t, f), BF),
            pltpu.VMEM((t, f), BF),
            pltpu.VMEM((t, f), BF),
            pltpu.VMEM((2, d, f), BF),
            pltpu.VMEM((2, d, f), BF),
            pltpu.VMEM((2, f, d), BF),
            sem((2,)), sem((2,)), sem((2,)), sem((2,)),
            *ring_scratch(z),
        ],
        compiler_params=pltpu.CompilerParams(vmem_limit_bytes=VMEM_LIMIT, collective_id=0, has_side_effects=True),
        cost_estimate=pl.CostEstimate(flops=16 * t * d * z.ff, bytes_accessed=60_000_000, transcendentals=t * z.ff),
        name="last_layer",
    )(a, y, h, wg, wu, wd)


def first_kernel(z, tm, depth, layer, a_hbm, y_hbm, act_hbm, slope_hbm, p_hbm, wd, sq_in, gu_out, d_out, from_d, sq_out,
                 a_v, y_v, p_v, gg_v, gu_v, wd_v, act_v, slope_v, every, in_sem, wd_sem, p_sem, act_sem, slope_sem, every_sem,
                 *ring_refs):
    ring = Ring(z, gu_out, d_out, from_d, dict(zip(RING_NAMES, ring_refs, strict=True)))
    tiles = z.tokens // tm

    def fetch(b, slot):
        for c in range(z.chips):
            cols = slice(c * LANES, (c + 1) * LANES)
            pltpu.make_async_copy(wd.at[layer, pl.ds(z.tile(c, b), LANES), :], wd_v.at[slot, cols, :], wd_sem.at[slot]).start()
        pltpu.make_async_copy(p_hbm.at[b], p_v.at[slot], p_sem.at[slot]).start()

    def tile_copies(q):
        b, r, s = q // tiles, rows_of(lax.rem(q, tiles), tm), lax.rem(q, depth)
        return (
            pltpu.make_async_copy(act_hbm.at[b, r, :], act_v.at[s], act_sem.at[s]),
            pltpu.make_async_copy(slope_hbm.at[b, r, :], slope_v.at[s], slope_sem.at[s]),
        )

    loads = (pltpu.make_async_copy(y_hbm, y_v, in_sem.at[1]), pltpu.make_async_copy(a_hbm, a_v, in_sem.at[0]))
    loads[0].start()
    fetch(0, 0)
    for q in range(depth - 1):
        for cp in tile_copies(q):
            cp.start()
    loads[1].start()
    ring.greet(True)
    for cp in loads:
        cp.wait()

    def compute(b):
        slot = lax.rem(b, 2)
        pltpu.make_async_copy(wd_v.at[slot], wd_v.at[slot], wd_sem.at[slot]).wait()
        pltpu.make_async_copy(p_hbm.at[b], p_v.at[slot], p_sem.at[slot]).wait()

        @pl.when(b + 1 < z.blocks)
        def _():
            fetch(b + 1, 1 - slot)

        def hidden(i, _):
            q = b * tiles + i
            for cp in tile_copies(q):
                cp.wait()

            @pl.when(q + depth - 1 < z.blocks * tiles)
            def _():
                for cp in tile_copies(q + depth - 1):
                    cp.start()

            r, s = rows_of(i, tm), lax.rem(q, depth)
            dp = dot(y_v[r, :], wd_v[slot], NT).astype(BF).astype(F32)
            gu_v[r, :] = (dp * act_v[s]).astype(BF)
            gg_v[r, :] = (dp * slope_v[s]).astype(BF)
            return 0

        lax.fori_loop(0, tiles, hidden, 0)
        weight_gradients(z, ring, slot, a_v, y_v, p_v[slot], gg_v[...], gu_v[...])

    def step(t, _):
        pl.when(t < z.blocks)(lambda: compute(t))
        ring.tick(t)
        return 0

    lax.fori_loop(0, z.blocks + 3, step, 0)

    me = lax.axis_index("dp")
    every[0] = ring.sq[...] + sq_in[...]
    out = []
    for i in range(1, z.devices):
        who = {"dp": lax.rem(me + i, z.devices)}
        out.append(pltpu.make_async_remote_copy(every.at[0], every.at[i], every_sem.at[0, i], every_sem.at[1, i],
                                                device_id=who, device_id_type=MESH))
        out[-1].start()
    ring.finish()
    for cp in out:
        cp.wait()
    total = jnp.zeros((8, LANES), F32)
    for i in range(z.devices):
        total += every[lax.rem(me - i + z.devices, z.devices)]
    sq_out[...] = total


def first_layer(z, layer, a, y, act, slope, p, wd, sq):
    tm, depth = z.tokens // 8, 4
    t, d, f = z.tokens, z.d, z.block
    any_, vmem = pl.BlockSpec(memory_space=pl.ANY), pl.BlockSpec(memory_space=pltpu.VMEM)
    sem = pltpu.SemaphoreType.DMA
    return pl.pallas_call(
        functools.partial(first_kernel, z, tm, depth, layer),
        out_shape=shard_shapes(z) + [jax.ShapeDtypeStruct((8, LANES), F32)],
        in_specs=[any_] * 6 + [vmem],
        out_specs=[vmem] * 4,
        scratch_shapes=[
            pltpu.VMEM((t, d), BF),
            pltpu.VMEM((t, d), BF),
            pltpu.VMEM((2, t, f), BF),
            pltpu.VMEM((t, f), BF),
            pltpu.VMEM((t, f), BF),
            pltpu.VMEM((2, f, d), BF),
            pltpu.VMEM((depth, tm, f), F32),
            pltpu.VMEM((depth, tm, f), F32),
            pltpu.VMEM((z.devices, 8, LANES), F32),
            sem((2,)), sem((2,)), sem((2,)), sem((depth,)), sem((depth,)), sem((2, z.devices)),
            *ring_scratch(z),
        ],
        compiler_params=pltpu.CompilerParams(vmem_limit_bytes=VMEM_LIMIT, collective_id=1, has_side_effects=True),
        cost_estimate=pl.CostEstimate(flops=8 * t * d * z.ff, bytes_accessed=130_000_000, transcendentals=0),
        name="first_layer",
    )(a, y, act, slope, p, wd, sq)


def adamw(w, m, v, g):
    m = 0.9 * m + 0.1 * g
    v = 0.95 * v + 0.05 * g * g
    step = m * lax.rsqrt(v + 1e-8) + 0.1 * w
    return (w - 0.02 * step).astype(BF), m, v


def gather(own, n, out, layer):
    rows = own.shape[0]
    me = lax.axis_index("dp")
    chip, core, chips = me // 2, me % 2, n // 2

    def send(a, by, other):
        to = lambda d: 2 * ((d // 2 + by) % chips) + (d % 2) ^ other
        return lax.ppermute(a, "dp", [(d, to(d)) for d in range(n)])

    def put(out, a, by, k, off=0):
        return lax.dynamic_update_slice(out, a[None], (layer, (2 * ((chip + by) % chips) + k) * rows + off, 0))

    half = rows // 2
    left, right = send(own, 1, 0), send(own, -1, 0)
    parts = [(own, 0, 0), (left, chips - 1, 0), (right, 1, 0), (send(left[:half], 1, 0), chips - 2, 0), (send(right[half:], -1, 0), chips - 2, half)]
    for a, by, off in parts:
        out = put(out, a, by, core, off)
        out = put(out, send(a, 0, 1), by, 1 - core, off)
    return out


def down_share(z, own, got):
    core = lax.rem(lax.axis_index("dp"), 2)
    n, r = z.blocks // 2, z.down_rows
    own = lax.dynamic_slice_in_dim(own, core * (n * r), (n + 1) * r, 0).reshape(n + 1, r, z.d)
    both = jnp.stack([own[:n], got.reshape(n, r, z.d)], 1).reshape(2 * n * r, z.d)
    return jnp.concatenate([both, own[n]], 0)


def solution(mesh):
    def step(x, dy, *arrays):
        weights, m, v = (arrays[i : i + 3] for i in (0, 3, 6))
        w_gate, w_up, w_down = weights
        z = Sizes(mesh, x, w_gate)
        n = z.devices
        x, dy = x[0], dy[0]
        h, a1, a0, act, slope, p = forward(z, 0, x, w_gate, w_up, w_down)
        dh, gu1, d1, from1, sq = last_layer(z, 1, a1, dy, h, w_gate, w_up, w_down)
        gu0, d0, from0, sq = first_layer(z, 0, a0, dh, act, slope, p, w_down, sq)
        factor = jnp.minimum(1.0, 0.5 * lax.rsqrt(jnp.sum(sq) / sum(w.size for w in weights) + 1e-30))
        shards = [(gu0[0], gu1[0]), (gu0[1], gu1[1]), (down_share(z, d0, from0), down_share(z, d1, from1))]
        me = lax.axis_index("dp")
        new = []
        for w, m_, v_, gs in zip(weights, m, v, shards, strict=True):
            rows = w.shape[1] // n
            out = jnp.zeros(w.shape, BF)
            ms, vs = [], []
            for l, g in enumerate(gs):
                own = lax.dynamic_slice(w, (l, me * rows, 0), (1, rows, w.shape[2]))[0].astype(F32)
                own, a, b = adamw(own, m_[l], v_[l], g.astype(F32) * factor)
                out = gather(own, n, out, l)
                ms.append(a)
                vs.append(b)
            new.append((out, jnp.stack(ms), jnp.stack(vs)))
        return tuple(one[which] for which in range(3) for one in new)

    data, whole, shard = P(("rep", "dp"), None, None), P(None, None, None), P(None, "dp", None)
    return jax.shard_map(
        step,
        mesh=mesh,
        in_specs=(data, data) + (whole,) * 3 + (shard,) * 6,
        out_specs=(P("rep", None, None),) * 3 + (P("rep", "dp", None),) * 6,
        check_vma=False,
    )
```

```python
import functools

import jax
import jax.numpy as jnp
from jax import lax
from jax.experimental import pallas as pl
from jax.experimental.pallas import tpu as pltpu
from jax.sharding import PartitionSpec as P

BF, F32 = jnp.bfloat16, jnp.float32
LANES = 128
MESH = pl.DeviceIdType.MESH
NN, NT, TN = ((1,), (0,)), ((1,), (1,)), ((0,), (0,))
VMEM_LIMIT = 67_000_000


def dot(a, b, dims):
    return lax.dot_general(a, b, (dims, ((), ())), preferred_element_type=F32)


def rows_of(i, n):
    return pl.ds(pl.multiple_of(i * n, n), n)


def scale_of(wide):
    return lax.rsqrt(jnp.mean(wide * wide, -1, keepdims=True) + 1e-6)


class Sizes:
    def __init__(self, mesh, x, w_gate):
        self.axes = mesh.axis_names
        self.devices = mesh.shape["dp"]
        self.chips = self.devices // 2
        self.tokens, self.d = x.shape[-2:]
        self.ff = w_gate.shape[-1]
        self.block = LANES * self.chips
        self.blocks = self.ff // self.block
        self.rows = self.d // self.devices
        self.down_rows = LANES // 2

    def tile(self, chip, b):
        return pl.multiple_of((self.blocks * chip + b) * LANES, LANES)


def forward_kernel(z, tm, layer, x_hbm, wg, wu, wd, h_out, a_out, a0_out, act_out, slope_out, p_out,
                   x_v, a_v, p_v, wg_v, wu_v, wd_v, act_v, slope_v, in_sem, wg_sem, wu_sem, wd_sem, act_sem, slope_sem, p_sem, out_sem):
    def fetch(b, slot):
        for c in range(z.chips):
            cols = slice(c * LANES, (c + 1) * LANES)
            pltpu.make_async_copy(wg.at[layer, :, pl.ds(z.tile(c, b), LANES)], wg_v.at[slot, :, cols], wg_sem.at[slot]).start()
            pltpu.make_async_copy(wu.at[layer, :, pl.ds(z.tile(c, b), LANES)], wu_v.at[slot, :, cols], wu_sem.at[slot]).start()

    load = pltpu.make_async_copy(x_hbm, x_v, in_sem)
    load.start()
    fetch(0, 0)
    for b in range(z.blocks):
        for c in range(z.chips):
            to = b * z.block + c * LANES
            pltpu.make_async_copy(wd.at[layer, pl.ds(z.tile(c, b), LANES), :], wd_v.at[to : to + LANES, :], wd_sem).start()
    load.wait()

    def norm(i, _):
        r = rows_of(i, 256)
        wide = x_v[r, :].astype(F32)
        a_v[r, :] = (wide * scale_of(wide)).astype(BF)
        return 0

    lax.fori_loop(0, z.tokens // 256, norm, 0)
    keep_a = pltpu.make_async_copy(a_v, a0_out, out_sem.at[0])
    keep_a.start()
    tiles = z.tokens // tm

    def stores(b, i, s):
        r = rows_of(i, tm)
        return (
            pltpu.make_async_copy(act_v.at[s], act_out.at[b, r, :], act_sem.at[s]),
            pltpu.make_async_copy(slope_v.at[s], slope_out.at[b, r, :], slope_sem.at[s]),
        )

    def block(b, _):
        slot = lax.rem(b, 2)
        pltpu.make_async_copy(wg_v.at[slot], wg_v.at[slot], wg_sem.at[slot]).wait()
        pltpu.make_async_copy(wu_v.at[slot], wu_v.at[slot], wu_sem.at[slot]).wait()

        @pl.when(b + 1 < z.blocks)
        def _():
            fetch(b + 1, 1 - slot)

        cols = pl.ds(pl.multiple_of(b * z.block, z.block), z.block)

        def pair(j, _):
            for s in range(2):
                i = 2 * j + s
                r = rows_of(i, tm)

                @pl.when(b + j > 0)
                def _():
                    for cp in stores(b, i, s):
                        cp.wait()

                gate = dot(a_v[r, :], wg_v[slot], NN)
                up = dot(a_v[r, :], wu_v[slot], NN)
                s_ = 1.0 / (1.0 + jnp.exp(-gate))
                act = gate * s_
                p_v[r, cols] = (act * up).astype(BF)
                act_v[s] = act
                slope_v[s] = up * (s_ + act * (1.0 - s_))
                for cp in stores(b, i, s):
                    cp.start()
            return 0

        lax.fori_loop(0, tiles // 2, pair, 0)
        pltpu.make_async_copy(p_v.at[:, cols], p_out.at[b], p_sem.at[b]).start()
        return 0

    lax.fori_loop(0, z.blocks, block, 0)
    for s in range(2):
        for cp in stores(0, 0, s):
            cp.wait()
    pltpu.make_async_copy(wd_v, wd_v, wd_sem).wait()
    keep_a.wait()

    def down(i, _):
        r = rows_of(i, tm // 2)
        out = dot(p_v[r, :], wd_v[...], NN).astype(BF)
        h = (x_v[r, :].astype(F32) + out.astype(F32)).astype(BF)
        x_v[r, :] = h
        wide = h.astype(F32)
        a_v[r, :] = (wide * scale_of(wide)).astype(BF)
        return 0

    lax.fori_loop(0, 2 * tiles, down, 0)
    last = (pltpu.make_async_copy(x_v, h_out, out_sem.at[1]), pltpu.make_async_copy(a_v, a_out, out_sem.at[2]))
    for cp in last:
        cp.start()
    for b in range(z.blocks):
        pltpu.make_async_copy(p_v.at[:, b * z.block : (b + 1) * z.block], p_out.at[b], p_sem.at[b]).wait()
    for cp in last:
        cp.wait()


def forward(z, layer, x, wg, wu, wd):
    tm = z.tokens // 2
    t, d, f, n = z.tokens, z.d, z.block, z.blocks
    any_ = pl.BlockSpec(memory_space=pl.ANY)
    sem = pltpu.SemaphoreType.DMA
    return pl.pallas_call(
        functools.partial(forward_kernel, z, tm, layer),
        out_shape=[jax.ShapeDtypeStruct((t, d), BF)] * 3
        + [jax.ShapeDtypeStruct((n, t, f), F32)] * 2
        + [jax.ShapeDtypeStruct((n, t, f), BF)],
        in_specs=[any_] * 4,
        out_specs=[any_] * 6,
        scratch_shapes=[
            pltpu.VMEM((t, d), BF),
            pltpu.VMEM((t, d), BF),
            pltpu.VMEM((t, z.ff), BF),
            pltpu.VMEM((2, d, f), BF),
            pltpu.VMEM((2, d, f), BF),
            pltpu.VMEM((z.ff, d), BF),
            pltpu.VMEM((2, tm, f), F32),
            pltpu.VMEM((2, tm, f), F32),
            sem, sem((2,)), sem((2,)), sem, sem((2,)), sem((2,)), sem((n,)), sem((3,)),
        ],
        compiler_params=pltpu.CompilerParams(vmem_limit_bytes=VMEM_LIMIT),
        cost_estimate=pl.CostEstimate(flops=6 * t * d * z.ff, bytes_accessed=150_000_000, transcendentals=t * z.ff),
        name="forward",
    )(x, wg, wu, wd)


class Ring:
    NAMES = ("st_gu", "st_d", "r0_gu", "r0_d", "s_gu", "s_d", "t1_gu", "t1_d", "r1_gu", "r1_d", "t2_gu", "t2_d", "r2_gu", "r2_d",
             "g_gu", "g_d", "give", "sq", "sem0", "sem1", "sem2", "g_sem", "swap_sem")

    @staticmethod
    def scratch(z):
        r, f, dr, d, n = z.rows, z.block, z.down_rows, z.d, z.chips
        sem = pltpu.SemaphoreType.DMA
        return [
            pltpu.VMEM((2, 2, n, 2, r, f), BF),
            pltpu.VMEM((2, n, 2, dr, d), BF),
            pltpu.VMEM((2, 2, n, r, f), BF),
            pltpu.VMEM((2, n, dr, d), BF),
            pltpu.VMEM((3, 3, 2, r, f), F32),
            pltpu.VMEM((3, 3, dr, d), F32),
            pltpu.VMEM((2, r, f), BF),
            pltpu.VMEM((2, dr // 2, d), BF),
            pltpu.VMEM((3, 2, r, f), BF),
            pltpu.VMEM((3, 2, dr // 2, d), BF),
            pltpu.VMEM((2, 2, r, f), BF),
            pltpu.VMEM((2, dr, d), BF),
            pltpu.VMEM((3, 2, 2, r, f), BF),
            pltpu.VMEM((3, 2, dr, d), BF),
            pltpu.VMEM((2, r, f), BF),
            pltpu.VMEM((dr, d), BF),
            pltpu.VMEM((2, z.blocks // 2, dr, d), BF),
            pltpu.VMEM((8, LANES), F32),
            sem((2, 2, 2)),
            sem((3, 2, 2, 2)),
            sem((3, 2, 2, 2)),
            sem((2,)),
            sem((2, 2)),
        ]

    def __init__(self, z, units, gu_out, d_out, refs):
        self.z, self.units, self.gu_out, self.d_out = z, units, gu_out, d_out
        self.__dict__.update(zip(self.NAMES, refs, strict=True))
        me = lax.axis_index("dp")
        self.chip, self.core = me // 2, lax.rem(me, 2)
        n = z.chips
        self.right = lax.rem(self.chip + 1, n)
        self.left = lax.rem(self.chip + n - 1, n)
        self.far = lax.rem(self.chip + 2, n)
        self.partner = {"dp": 2 * self.chip + 1 - self.core}
        self.sides = ({"dp": 2 * self.right + self.core}, {"dp": 2 * self.left + self.core})

    def greet(self):
        barrier, n = pltpu.get_barrier_semaphore(), self.z.devices
        for i in range(1, n):
            pl.semaphore_signal(barrier, inc=1, device_id={"dp": lax.rem(lax.axis_index("dp") + i, n)}, device_id_type=MESH)
        pl.semaphore_wait(barrier, n - 1)
        self.sq[...] = jnp.zeros_like(self.sq)

    def remote(self, src, dst, sems, who):
        return pltpu.make_async_remote_copy(src, dst, sems.at[0], sems.at[1], device_id=who, device_id_type=MESH)

    def copies0(self, u):
        s, other = lax.rem(u, 2), 1 - self.core
        return (
            self.remote(self.st_gu.at[s, :, :, other], self.r0_gu.at[s], self.sem0.at[s, 0], self.partner),
            self.remote(self.st_d.at[s, :, other], self.r0_d.at[s], self.sem0.at[s, 1], self.partner),
        )

    def copies1(self, u):
        s, out = lax.rem(u, 3), []
        for way in range(2):
            out.append(self.remote(self.t1_gu.at[way], self.r1_gu.at[s, way], self.sem1.at[s, way, 0], self.sides[way]))
            out.append(self.remote(self.t1_d.at[way], self.r1_d.at[s, way], self.sem1.at[s, way, 1], self.sides[way]))
        return out

    def copies2(self, u):
        s, out = lax.rem(u, 3), []
        for way in range(2):
            out.append(self.remote(self.t2_gu.at[way], self.r2_gu.at[s, way], self.sem2.at[s, way, 0], self.sides[way]))
            out.append(self.remote(self.t2_d.at[way], self.r2_d.at[s, way], self.sem2.at[s, way, 1], self.sides[way]))
        return out

    def share_copies(self, u):
        z = self.z
        layer, b = 1 - u // z.blocks, lax.rem(u, z.blocks)
        out = []
        for c in range(z.chips):
            cols = slice(c * LANES, (c + 1) * LANES)
            out.append(pltpu.make_async_copy(self.g_gu.at[:, :, cols], self.gu_out.at[layer, :, :, pl.ds(z.tile(c, b), LANES)], self.g_sem.at[0]))
        place = b - self.core * (z.blocks // 2)
        own = (place >= 0) & (place <= z.blocks // 2)
        mine = pltpu.make_async_copy(self.g_d, self.d_out.at[layer, jnp.clip(place, 0, z.blocks // 2), 0], self.g_sem.at[1])
        return out, own, mine

    def stage0(self, u):
        for cp in self.copies0(u):
            cp.start()

    def stage1(self, u):
        for cp in self.copies0(u):
            cp.wait()

        @pl.when(u > 0)
        def _():
            for cp in self.copies1(u - 1):
                cp.wait_send()

        k, r, s = self.core, lax.rem(u, 2), lax.rem(u, 3)
        half = self.z.down_rows // 2
        for w in range(2):
            self.t1_gu[w] = (self.st_gu[r, w, self.far, k].astype(F32) + self.r0_gu[r, w, self.far].astype(F32)).astype(BF)
            h = slice(w * half, (w + 1) * half)
            self.t1_d[w] = (self.st_d[r, self.far, k, h].astype(F32) + self.r0_d[r, self.far, h].astype(F32)).astype(BF)
        for cp in self.copies1(u):
            cp.start()
        for at, chip in enumerate((self.right, self.left, self.chip)):
            for w in range(2):
                self.s_gu[s, at, w] = self.st_gu[r, w, chip, k].astype(F32) + self.r0_gu[r, w, chip].astype(F32)
            self.s_d[s, at] = self.st_d[r, chip, k].astype(F32) + self.r0_d[r, chip].astype(F32)

    def stage2(self, u):
        for cp in self.copies1(u):
            cp.wait_recv()

        @pl.when(u > 0)
        def _():
            for cp in self.copies2(u - 1):
                cp.wait_send()

        s = lax.rem(u, 3)
        half = self.z.down_rows // 2
        for way in range(2):
            w, v = way, 1 - way
            self.t2_gu[way, w] = (self.s_gu[s, way, w] + self.r1_gu[s, way].astype(F32)).astype(BF)
            self.t2_gu[way, v] = self.s_gu[s, way, v].astype(BF)
            h, o = slice(w * half, (w + 1) * half), slice(v * half, (v + 1) * half)
            self.t2_d[way, h] = (self.s_d[s, way, h] + self.r1_d[s, way].astype(F32)).astype(BF)
            self.t2_d[way, o] = self.s_d[s, way, o].astype(BF)
        for cp in self.copies2(u):
            cp.start()

    def wait_share(self, u):
        tiles, own, mine = self.share_copies(u)
        for cp in tiles:
            cp.wait()
        pl.when(own)(mine.wait)

    def stage3(self, u):
        z, s = self.z, lax.rem(u, 3)
        for cp in self.copies2(u):
            cp.wait_recv()
        pl.when(u > 0)(lambda: self.wait_share(u - 1))
        total = self.sq[...]
        for w in range(2):
            g = (self.s_gu[s, 2, w] + self.r2_gu[s, 0, w].astype(F32) + self.r2_gu[s, 1, w].astype(F32)).astype(BF)
            self.g_gu[w] = g
            total += self.squares(g)
        g = (self.s_d[s, 2] + self.r2_d[s, 0].astype(F32) + self.r2_d[s, 1].astype(F32)).astype(BF)
        self.sq[...] = total + self.squares(g)
        tiles, own, mine = self.share_copies(u)

        @pl.when(own)
        def _():
            self.g_d[...] = g
            mine.start()

        @pl.when(~own)
        def _():
            b = lax.rem(u, z.blocks)
            self.give[1 - u // z.blocks, jnp.clip(b - (1 - self.core) * (z.blocks // 2 + 1), 0, z.blocks // 2 - 1)] = g

        for cp in tiles:
            cp.start()

    @staticmethod
    def squares(g):
        parts = []
        for j in range(0, g.shape[1], LANES):
            wide = g[:, j : j + LANES].astype(F32)
            wide = wide * wide
            total = wide[0:8]
            for i in range(8, g.shape[0], 8):
                total += wide[i : i + 8]
            parts.append(total)
        return sum(parts[1:], parts[0])

    def first(self, t):
        turn = self.z.blocks - 1
        u = jnp.where(t - 2 < turn, t - 2, t - 4)
        pl.when((u >= 0) & ((t - 2 < turn) | (u >= turn)) & (u < self.units))(lambda: self.stage3(u))
        pl.when((t >= 1) & (t - 1 <= turn))(lambda: self.stage1(t - 1))

    def second(self, t):
        turn = self.z.blocks - 1
        pl.when((t - 1 > turn) & (t - 1 < self.units))(lambda: self.stage1(t - 1))
        u = jnp.where(t - 1 < turn, t - 1, t - 2)
        pl.when((u >= 0) & ((t - 1 < turn) | (u >= turn)) & (u < self.units))(lambda: self.stage2(u))

    def third(self, t):
        self.stage0(t)

    def swaps(self):
        n = self.z.blocks // 2
        return [self.remote(self.give.at[l], self.d_out.at[l, pl.ds(0, n), 1], self.swap_sem.at[l], self.partner) for l in range(2)]

    def finish(self):
        for cp in (*self.copies1(self.units - 1), *self.copies2(self.units - 1)):
            cp.wait_send()
        self.wait_share(self.units - 1)
        for cp in self.swaps():
            cp.wait()


def backward_kernel(z, tm, a1_hbm, a0_hbm, y_hbm, h_hbm, act_hbm, slope_hbm, p_hbm, wg, wu, wd, gu_out, d_out, sq_out,
                    a_v, y_v, da_v, p_v, gg_v, gu_v, wg_v, wu_v, wd_v, every,
                    a_sem, y_sem, wg_sem, wu_sem, wd_sem, p_sem, act_sem, slope_sem, every_sem, *ring_refs):
    nb = z.blocks
    ring = Ring(z, 2 * nb, gu_out, d_out, ring_refs)
    long = z.tokens // 2

    def fetch_down(layer, b, slot):
        for c in range(z.chips):
            rows = slice(c * LANES, (c + 1) * LANES)
            pltpu.make_async_copy(wd.at[layer, pl.ds(z.tile(c, b), LANES), :], wd_v.at[slot, rows, :], wd_sem.at[slot]).start()

    def fetch(b, slot):
        for c in range(z.chips):
            cols = slice(c * LANES, (c + 1) * LANES)
            pltpu.make_async_copy(wg.at[1, :, pl.ds(z.tile(c, b), LANES)], wg_v.at[slot, :, cols], wg_sem.at[slot]).start()
            pltpu.make_async_copy(wu.at[1, :, pl.ds(z.tile(c, b), LANES)], wu_v.at[slot, :, cols], wu_sem.at[slot]).start()
        fetch_down(1, b, slot)

    def slot_wait(v, sem, slot):
        pltpu.make_async_copy(v.at[slot], v.at[slot], sem.at[slot]).wait()

    def saved(b):
        out = []
        for i in range(2):
            r = pl.ds(i * long, long)
            out.append(pltpu.make_async_copy(act_hbm.at[b, r, :], da_v.at[r, 0 : z.block], act_sem.at[i]))
            out.append(pltpu.make_async_copy(slope_hbm.at[b, r, :], da_v.at[r, z.block : 2 * z.block], slope_sem.at[i]))
        return out

    def p_load(b):
        return pltpu.make_async_copy(p_hbm.at[b], p_v, p_sem)

    loads = (pltpu.make_async_copy(a1_hbm, a_v, a_sem), pltpu.make_async_copy(y_hbm, y_v, y_sem))
    for cp in loads:
        cp.start()
    fetch(0, 0)
    ring.greet()
    da_v[...] = jnp.zeros_like(da_v)
    for cp in loads:
        cp.wait()

    def down_gradient(slot):
        ring.st_d[slot] = dot(p_v[...], y_v[...], TN).astype(BF).reshape(z.chips, 2, z.down_rows, z.d)

    def up_gradients(slot):
        ring.st_gu[slot, 0] = dot(a_v[...], gg_v[...], TN).astype(BF).reshape(z.chips, 2, z.rows, z.block)
        ring.st_gu[slot, 1] = dot(a_v[...], gu_v[...], TN).astype(BF).reshape(z.chips, 2, z.rows, z.block)

    def last_hidden(b):
        slot = lax.rem(b, 2)
        for v, sem in ((wg_v, wg_sem), (wu_v, wu_sem), (wd_v, wd_sem)):
            slot_wait(v, sem, slot)
        pl.when(b + 1 < nb)(lambda: fetch(b + 1, 1 - slot))
        pl.when(b + 1 == nb)(lambda: fetch_down(0, 0, 1 - slot))

        def tile(i, _):
            r = rows_of(i, tm)
            gate = dot(a_v[r, :], wg_v[slot], NN)
            up = dot(a_v[r, :], wu_v[slot], NN)
            dp = dot(y_v[r, :], wd_v[slot], NT).astype(BF).astype(F32)
            s_ = 1.0 / (1.0 + jnp.exp(-gate))
            act = gate * s_
            p_v[r, :] = (act * up).astype(BF)
            gu_v[r, :] = (dp * act).astype(BF)
            gg_v[r, :] = (dp * (up * (s_ + act * (1.0 - s_)))).astype(BF)
            return 0

        lax.fori_loop(0, z.tokens // tm, tile, 0)

    def last_back(b):
        slot = lax.rem(b, 2)
        h_load = pltpu.make_async_copy(h_hbm, a_v, a_sem)
        pl.when(b + 1 == nb)(h_load.start)

        def back(i, _):
            r = rows_of(i, long)
            for c in (slice(0, 5 * LANES), slice(5 * LANES, z.d)):
                da_v[r, c] += dot(gg_v[r, :], wg_v[slot, c], NT) + dot(gu_v[r, :], wu_v[slot, c], NT)
            return 0

        lax.fori_loop(0, z.tokens // long, back, 0)

        @pl.when(b + 1 == nb)
        def _():
            h_load.wait()
            lax.fori_loop(0, z.tokens // 256, through_norm, 0)
            for cp in saved(0):
                cp.start()
            pltpu.make_async_copy(a0_hbm, a_v, a_sem).start()

    def through_norm(i, _):
        r = rows_of(i, 256)
        wide = a_v[r, :].astype(F32)
        scale = scale_of(wide)
        da = da_v[r, :].astype(BF).astype(F32)
        pull = jnp.sum(da * wide, -1, keepdims=True) * (scale * scale * scale) * (1.0 / z.d)
        dh = (da * scale - wide * pull).astype(BF)
        y_v[r, :] = (y_v[r, :].astype(F32) + dh.astype(F32)).astype(BF)
        return 0

    def first_hidden(t):
        b, slot = t - nb, lax.rem(t, 2)
        slot_wait(wd_v, wd_sem, slot)
        pl.when(b + 1 < nb)(lambda: fetch_down(0, b + 1, 1 - slot))
        for cp in saved(b):
            cp.wait()

        def tile(i, _):
            r = rows_of(i, tm)
            dp = dot(y_v[r, :], wd_v[slot], NT).astype(BF).astype(F32)
            gu_v[r, :] = (dp * da_v[r, 0 : z.block]).astype(BF)
            gg_v[r, :] = (dp * da_v[r, z.block : 2 * z.block]).astype(BF)
            return 0

        lax.fori_loop(0, z.tokens // tm, tile, 0)

        @pl.when(b + 1 < nb)
        def _():
            for cp in saved(b + 1):
                cp.start()

    def gradients(t):
        slot = lax.rem(t, 2)
        pl.when(t >= nb)(lambda: p_load(t - nb).wait())
        pl.when(t == nb)(pltpu.make_async_copy(a0_hbm, a_v, a_sem).wait)
        down_gradient(slot)
        up_gradients(slot)
        pl.when((t + 1 >= nb) & (t + 1 < 2 * nb))(lambda: p_load(t + 1 - nb).start())
        ring.third(t)

    def step(t, _):
        ring.first(t)
        pl.when(t < nb)(lambda: last_hidden(t))
        pl.when((t >= nb) & (t < 2 * nb))(lambda: first_hidden(t))
        ring.second(t)
        pl.when(t < 2 * nb)(lambda: gradients(t))
        pl.when(t < nb)(lambda: last_back(t))
        return 0

    lax.fori_loop(0, 2 * nb + 4, step, 0)

    me, n = lax.axis_index("dp"), z.devices
    every[0] = ring.sq[...]
    out = [ring.remote(every.at[0], every.at[i], every_sem.at[i], {"dp": lax.rem(me + i, n)}) for i in range(1, n)]
    for cp in (*out, *ring.swaps()):
        cp.start()
    ring.finish()
    for cp in out:
        cp.wait()
    total = jnp.zeros((8, LANES), F32)
    for i in range(n):
        total += every[lax.rem(me - i + n, n)]
    sq_out[...] = total


def backward(z, a1, a0, y, h, act, slope, p, wg, wu, wd):
    tm = z.tokens // 4
    t, d, f = z.tokens, z.d, z.block
    any_, vmem = pl.BlockSpec(memory_space=pl.ANY), pl.BlockSpec(memory_space=pltpu.VMEM)
    sem = pltpu.SemaphoreType.DMA
    return pl.pallas_call(
        functools.partial(backward_kernel, z, tm),
        out_shape=[
            jax.ShapeDtypeStruct((2, 2, z.rows, z.ff), BF),
            jax.ShapeDtypeStruct((2, z.blocks // 2 + 1, 2, z.down_rows, d), BF),
            jax.ShapeDtypeStruct((8, LANES), F32),
        ],
        in_specs=[any_] * 10,
        out_specs=[any_, any_, vmem],
        scratch_shapes=[
            pltpu.VMEM((t, d), BF),
            pltpu.VMEM((t, d), BF),
            pltpu.VMEM((t, d), F32),
            pltpu.VMEM((t, f), BF),
            pltpu.VMEM((t, f), BF),
            pltpu.VMEM((t, f), BF),
            pltpu.VMEM((2, d, f), BF),
            pltpu.VMEM((2, d, f), BF),
            pltpu.VMEM((2, f, d), BF),
            pltpu.VMEM((z.devices, 8, LANES), F32),
            sem, sem, sem((2,)), sem((2,)), sem((2,)), sem, sem((2,)), sem((2,)), sem((z.devices, 2)),
            *Ring.scratch(z),
        ],
        compiler_params=pltpu.CompilerParams(vmem_limit_bytes=VMEM_LIMIT, collective_id=0, has_side_effects=True),
        cost_estimate=pl.CostEstimate(flops=24 * t * d * z.ff, bytes_accessed=200_000_000, transcendentals=t * z.ff),
        name="backward",
    )(a1, a0, y, h, act, slope, p, wg, wu, wd)


def adamw(w, m, v, g):
    m = 0.9 * m + 0.1 * g
    v = 0.95 * v + 0.05 * g * g
    step = m * lax.rsqrt(v + 1e-8) + 0.1 * w
    return (w - 0.02 * step).astype(BF), m, v


def optimizer_kernel(layer, which, chunks, count, sq, w_hbm, m_hbm, v_hbm, g_hbm, *refs):
    own_out, m_out, v_out, w_v, m_v, v_v, g_v, own_v, in_sem, out_sem = refs[-10:]
    rows = m_hbm.shape[1]
    part = rows // chunks
    at = pl.multiple_of(lax.axis_index("dp") * rows, rows)

    def loads(i):
        r = slice(i * part, (i + 1) * part)
        return (
            pltpu.make_async_copy(w_hbm.at[layer, pl.ds(at + i * part, part), :], w_v.at[r, :], in_sem.at[i, 0]),
            pltpu.make_async_copy(m_hbm.at[layer, r, :], m_v.at[r, :], in_sem.at[i, 1]),
            pltpu.make_async_copy(v_hbm.at[layer, r, :], v_v.at[r, :], in_sem.at[i, 2]),
            pltpu.make_async_copy(g_hbm.at[which, r, :], g_v.at[r, :], in_sem.at[i, 3]),
        )

    def stores(i):
        r = slice(i * part, (i + 1) * part)
        return (
            pltpu.make_async_copy(own_v.at[r, :], own_out.at[r, :], out_sem.at[i, 0]),
            pltpu.make_async_copy(m_v.at[r, :], m_out.at[layer, r, :], out_sem.at[i, 1]),
            pltpu.make_async_copy(v_v.at[r, :], v_out.at[layer, r, :], out_sem.at[i, 2]),
        )

    for i in range(chunks):
        for cp in loads(i):
            cp.start()
    factor = jnp.minimum(1.0, 0.5 * lax.rsqrt(jnp.sum(sq[...], keepdims=True) / count + 1e-30))
    for i in range(chunks):
        for cp in loads(i):
            cp.wait()

        def body(j, _):
            r = pl.ds(pl.multiple_of(i * part + j * 16, 16), 16)
            g = g_v[r, :].astype(F32) * factor
            own_v[r, :], m_v[r, :], v_v[r, :] = adamw(w_v[r, :].astype(F32), m_v[r, :], v_v[r, :], g)
            return 0

        lax.fori_loop(0, part // 16, body, 0)
        for cp in stores(i):
            cp.start()
    for i in range(chunks):
        for cp in stores(i):
            cp.wait()


def optimizer(layer, which, count, sq, w, m, v, g, before):
    _, rows, cols = m.shape
    chunks = 3
    any_, vmem = pl.BlockSpec(memory_space=pl.ANY), pl.BlockSpec(memory_space=pltpu.VMEM)
    sem = pltpu.SemaphoreType.DMA
    return pl.pallas_call(
        functools.partial(optimizer_kernel, layer, which, chunks, count),
        out_shape=[jax.ShapeDtypeStruct((rows, cols), BF)] + [jax.ShapeDtypeStruct(m.shape, F32)] * 2,
        in_specs=[vmem] + [any_] * (4 + len(before)),
        out_specs=[any_] * 3,
        input_output_aliases={5 + i: 1 + i for i in range(len(before))},
        scratch_shapes=[
            pltpu.VMEM((rows, cols), BF),
            pltpu.VMEM((rows, cols), F32),
            pltpu.VMEM((rows, cols), F32),
            pltpu.VMEM((rows, cols), BF),
            pltpu.VMEM((rows, cols), BF),
            sem((chunks, 4)),
            sem((chunks, 3)),
        ],
        compiler_params=pltpu.CompilerParams(vmem_limit_bytes=VMEM_LIMIT),
        cost_estimate=pl.CostEstimate(flops=12 * rows * cols, bytes_accessed=22 * rows * cols, transcendentals=rows * cols),
        name="optimizer",
    )(sq, w, m, v, g, *before)


def nothing(shape):
    return pl.pallas_call(
        lambda out: None, out_shape=jax.ShapeDtypeStruct(shape, BF), out_specs=pl.BlockSpec(memory_space=pl.ANY), name="nothing"
    )()


def place_kernel(layer, rows, spots, n, *refs):
    blocks, out, bufs = refs[: len(spots)], refs[len(spots) + 1], refs[len(spots) + 2 : -2]
    in_sem, out_sem = refs[-2:]
    me = lax.axis_index("dp")
    loads, stores = [], []
    for i, (block, buf, (by, other, off)) in enumerate(zip(blocks, bufs, spots, strict=True)):
        owner = 2 * lax.rem(me // 2 + by, n // 2) + (1 - lax.rem(me, 2) if other else lax.rem(me, 2))
        to = pl.multiple_of(owner * rows + off, 8)
        loads.append(pltpu.make_async_copy(block, buf, in_sem.at[i]))
        stores.append(pltpu.make_async_copy(buf, out.at[layer, pl.ds(to, block.shape[0]), :], out_sem.at[i]))
        loads[-1].start()
    for load, store in zip(loads, stores, strict=True):
        load.wait()
        store.start()
    for store in stores:
        store.wait()


def place(out, layer, rows, n, parts):
    blocks, spots = [p[0] for p in parts], [p[1:] for p in parts]
    any_ = pl.BlockSpec(memory_space=pl.ANY)
    sem = pltpu.SemaphoreType.DMA((len(parts),))
    size = sum(2 * b.size for b in blocks)
    return pl.pallas_call(
        functools.partial(place_kernel, layer, rows, spots, n),
        out_shape=jax.ShapeDtypeStruct(out.shape, out.dtype),
        in_specs=[any_] * (len(parts) + 1),
        out_specs=any_,
        input_output_aliases={len(parts): 0},
        scratch_shapes=[*(pltpu.VMEM(b.shape, b.dtype) for b in blocks), sem, sem],
        compiler_params=pltpu.CompilerParams(vmem_limit_bytes=VMEM_LIMIT),
        cost_estimate=pl.CostEstimate(flops=size // 2, bytes_accessed=2 * size, transcendentals=0),
        name="place",
    )(*blocks, out)


class Gather:
    def __init__(self, own, n, layer):
        self.n, self.layer, self.rows, self.half = n, layer, own.shape[0], own.shape[0] // 2
        self.chips = n // 2
        self.own = own
        self.left, self.right, self.mate = self.send(own, 1, 0), self.send(own, -1, 0), self.send(own, 0, 1)

    def send(self, a, by, other):
        to = lambda d: 2 * ((d // 2 + by) % self.chips) + (d % 2) ^ other
        return lax.ppermute(a, "dp", [(d, to(d)) for d in range(self.n)])

    def forward(self):
        self.far = self.send(self.left[: self.half], 1, 0), self.send(self.right[self.half :], -1, 0)
        self.mates = self.send(self.left, 0, 1), self.send(self.right, 0, 1)

    def pass_on(self):
        self.far_mates = tuple(self.send(a, 0, 1) for a in self.far)

    def near(self):
        return [(self.own, 0, 0, 0), (self.mate, 0, 1, 0), (self.left, self.chips - 1, 0, 0), (self.right, 1, 0, 0)]

    def beside(self):
        return [(self.mates[0], self.chips - 1, 1, 0), (self.mates[1], 1, 1, 0)]

    def distant(self, which, other):
        return [(a, self.chips - 2, other, i * self.half) for i, a in enumerate(which)]


def solution(mesh):
    def step(x, dy, *arrays):
        weights, m, v = (arrays[i : i + 3] for i in (0, 3, 6))
        w_gate, w_up, w_down = weights
        z = Sizes(mesh, x, w_gate)
        n = z.devices
        x, dy = x[0], dy[0]
        h, a1, a0, act, slope, p = forward(z, 0, x, w_gate, w_up, w_down)
        gu, d, sq = backward(z, a1, a0, dy, h, act, slope, p, w_gate, w_up, w_down)
        count = sum(w.size for w in weights)
        gu, d = gu.reshape(-1, z.rows, z.ff), d.reshape(2, -1, z.d)
        pieces = [(i, l) for i in range(3) for l in range(2)]
        outs = [nothing(w.shape) for w in weights]
        moments = [(), (), ()]
        going = []
        for i, l in pieces:
            g, which = (gu, 2 * l + i) if i < 2 else (d, l)
            own, *moments[i] = optimizer(l, which, count, sq, weights[i], m[i], v[i], g, moments[i])
            going.append(Gather(own, n, l))

        def settle(at, parts):
            i, l = pieces[at]
            outs[i] = place(outs[i], l, going[at].rows, n, parts)

        for at, piece in enumerate(going):
            if at:
                piece.left, piece.right, *outs = lax.optimization_barrier((piece.left, piece.right, *outs))
            piece.forward()
            settle(at, piece.near())
            if at:
                settle(at - 1, going[at - 1].beside())
        settle(at, piece.beside())
        for at, piece in enumerate(going):
            if at:
                *piece.far, outs[0], outs[1], outs[2] = lax.optimization_barrier((*piece.far, *outs))
            piece.pass_on()
            settle(at, piece.distant(piece.far, 0))
            if at:
                settle(at - 1, going[at - 1].distant(going[at - 1].far_mates, 1))
        settle(at, piece.distant(piece.far_mates, 1))
        return (*outs, *(mv[0] for mv in moments), *(mv[1] for mv in moments))

    data, whole, shard = P(("rep", "dp"), None, None), P(None, None, None), P(None, "dp", None)
    return jax.shard_map(
        step,
        mesh=mesh,
        in_specs=(data, data) + (whole,) * 3 + (shard,) * 6,
        out_specs=(P("rep", None, None),) * 3 + (P("rep", "dp", None),) * 6,
        check_vma=False,
    )
```
